32 devices in a mesh: head: 4 (over y, core), seq: 8 (over z, x).
Axes of the slice: x: 2, y: 2, z: 4, core: 2. Of those that a mesh axis runs over, the one named last changes fastest.
Arguments:
- cached_keys: bfloat16 [8, 32768, 8, 128], P(None, 'seq', 'head'), may hold values from -6 to 6
- queries: bfloat16 [8, 64, 128], P('seq', 'head'), may hold values from -6 to 6
- seq_lengths: int32 [8], replicated, may hold values from 1 to 32768
Outputs:
- page_min: bfloat16 [8, 2048, 8, 128], P('seq', 'head')
- page_max: bfloat16 [8, 2048, 8, 128], P('seq', 'head')
- page_mean: float32 [8, 2048, 8, 128], P('seq', 'head')
- page_score: float32 [8, 64, 2048], P('seq', None, 'head')
The draws below stay inside these ranges and needn't reach their ends.
All inputs are finite; a program needn't handle non-finite values.
Results may differ from the reference program's by a relative error of at most 0.001.
Values may be sent and summed in bfloat16 or wider, within the bound.
A program may use at most 192 MiB of HBM per device.

```python
import jax
import jax.numpy as jnp
from jax import lax

KVH = 8
QH = 64
HD = 128
PAGE = 16
LEN = 32768
SEQS = 8


def plant(values, key, smallest, high):
    longest = values.shape.index(max(values.shape))
    spots = []
    for shift in (0, 1):
        where = [jax.random.randint(jax.random.fold_in(key, axis), (), 0, length) for axis, length in enumerate(values.shape)]
        where[longest] = (where[longest] + shift) % values.shape[longest]
        spots.append(tuple(where))
    return values.at[spots[0]].set(smallest).at[spots[1]].set(high)


def block_levels(rng, shape, pieces, smallest, largest):
    def one(dim, parts):
        draws = jax.random.uniform(jax.random.fold_in(jax.random.fold_in(rng, 6), dim), (parts,), jnp.float32, smallest / len(pieces), largest / len(pieces))
        return jnp.repeat(jnp.exp(draws), shape[dim] // parts).reshape((-1,) + (1,) * (len(shape) - dim - 1))

    level = one(*pieces[0])
    for cut in pieces[1:]:
        level = level * one(*cut)
    return level


def noise(rng, shape, scale, most, split=(), held_as=jnp.bfloat16):
    result = scale * jax.random.normal(rng, shape, jnp.float32)
    if split:
        result = result * block_levels(rng, shape, split, -0.22, 0.18)
    return jnp.clip(result, -most, most).astype(held_as)


def setup_inputs(seed: int = 0) -> dict:
    key_list = jax.random.split(jax.random.key(seed), 4)
    return {
        "cached_keys": noise(key_list[0], (SEQS, LEN, KVH, HD), 1.0, 6.0, ((1, 8), (2, 4))),
        "queries": noise(key_list[1], (SEQS, QH, HD), 1.0, 6.0, ((0, 8), (1, 4))),
        "seq_lengths": plant(jax.random.randint(key_list[2], (SEQS,), 1, LEN + 1), jax.random.fold_in(key_list[2], 1), 1, LEN).astype(jnp.int32),
    }


def page_bounds(block, start, limit):
    seq_count = block.shape[0]
    tokens = block.shape[1]
    position = start + jnp.arange(tokens, dtype=jnp.int32)
    live_token = (position[None, :] < limit[:, None])[:, :, None, None]
    shaped = (seq_count, tokens // PAGE, PAGE, block.shape[2], block.shape[3])
    top_value = jnp.array(jnp.inf, block.dtype)
    lower = jnp.min(jnp.where(live_token, block, top_value).reshape(shaped), axis=2)
    upper = jnp.max(jnp.where(live_token, block, -top_value).reshape(shaped), axis=2)
    key_sums = jnp.sum(jnp.where(live_token, block, jnp.zeros((), block.dtype)).reshape(shaped), axis=2, dtype=jnp.float32)
    page_start = start + PAGE * jnp.arange(tokens // PAGE, dtype=jnp.int32)
    page_live = (page_start[None, :] < limit[:, None])[:, :, None, None]
    zero_value = jnp.zeros((), block.dtype)
    lower = jnp.where(page_live, lower, zero_value)
    upper = jnp.where(page_live, upper, zero_value)
    return lower, upper, key_sums


def page_average(key_sums, start, limit):
    page_start = start + PAGE * jnp.arange(key_sums.shape[1], dtype=jnp.int32)
    counts = jnp.clip(limit[:, None] - page_start[None, :], 0, PAGE).astype(jnp.float32)
    return key_sums / jnp.maximum(counts, 1.0)[:, :, None, None]


def bound_scores(query, lower, upper):
    seq_count, heads, width = query.shape
    kv_heads = lower.shape[2]
    grouped = query.astype(jnp.float32).reshape(seq_count, kv_heads, heads // kv_heads, width)
    positive = jnp.maximum(grouped, 0.0)
    negative = jnp.minimum(grouped, 0.0)
    score = jnp.einsum("shgc,sphc->shgp", positive, upper.astype(jnp.float32), precision=lax.Precision.HIGHEST)
    score = score + jnp.einsum("shgc,sphc->shgp", negative, lower.astype(jnp.float32), precision=lax.Precision.HIGHEST)
    return score.reshape(seq_count, heads, lower.shape[1]) * (width ** -0.5)


def one_sequence(inputs):
    block, limit, query = inputs
    limit = limit.reshape(1)
    lower, upper, key_sums = page_bounds(block[None], jnp.int32(0), limit)
    average = page_average(key_sums, jnp.int32(0), limit)
    score = bound_scores(query[None], lower, upper)
    return lower[0], upper[0], average[0], score[0]


def reference(cached_keys, queries, seq_lengths):
    lower, upper, average, score = lax.map(one_sequence, (cached_keys, seq_lengths, queries))
    return (lower, upper, average, score)
```

```python
import functools

import jax
import jax.numpy as jnp
from jax import lax
from jax.experimental import pallas as pl
from jax.experimental.pallas import tpu as pltpu
from jax.sharding import PartitionSpec as P

PAGE = 16
SLOTS = 3
MESH = pl.DeviceIdType.MESH
SPAN = 28.0
TOP = 32767.0


def page_kernel(
    seqs, heads, lengths, keys, query, low_out, high_out, sum_out, query_out,
    buf, low, high, code, key_sem, send_sem, recv_sem, own_sem, query_send, query_recv, query_own,
):
    head = lax.axis_index("head")
    seq = lax.axis_index("seq")
    ratio = seqs // heads
    pages = keys.shape[1]
    width = keys.shape[3]
    lanes = keys.shape[4]
    rows = pages * width
    chunk = min(64, rows)
    owner = seq // ratio
    part = lax.rem(seq, ratio)
    mine = owner == head

    def dest_of(step):
        return lax.rem(seq + lax.rem(step + seqs // 2, seqs), seqs)

    def fetch(step):
        slot = lax.rem(step, SLOTS)
        dest = dest_of(step)
        for t in range(PAGE):
            pltpu.make_async_copy(keys.at[dest, :, t], buf.at[slot, t], key_sem.at[slot, t]).start()

    for step in range(min(SLOTS - 1, seqs)):
        fetch(jnp.int32(step))

    barrier = pltpu.get_barrier_semaphore()

    def greet(i, carry):
        source_head = i // ratio
        source_seq = head * ratio + lax.rem(i, ratio)

        @pl.when(jnp.logical_or(source_head != head, source_seq != seq))
        def _():
            pl.semaphore_signal(barrier, inc=1, device_id=(source_head, source_seq), device_id_type=MESH)

        return carry

    lax.fori_loop(0, seqs, greet, 0)
    for i in range(1, heads):
        pl.semaphore_signal(barrier, inc=1, device_id=(lax.rem(head + i, heads), seq), device_id_type=MESH)
    expected = seqs - jnp.where(mine, 1, 0) + heads - 1
    pl.semaphore_wait(barrier, expected)

    def query_copy(i, target):
        return pltpu.make_async_remote_copy(
            src_ref=query, dst_ref=query_out.at[head], send_sem=query_send.at[i], recv_sem=query_recv.at[i],
            device_id=(target, seq), device_id_type=MESH,
        )

    for i in range(heads - 1):
        query_copy(i, lax.rem(head + i + 1, heads)).start()
    own_query = pltpu.make_async_copy(query, query_out.at[head], query_own)
    own_query.start()

    trio = ((low, low_out), (high, high_out), (code, sum_out))
    index = head * ratio + part

    def remote(step, k):
        source, target = trio[k]
        return pltpu.make_async_remote_copy(
            src_ref=source.at[step],
            dst_ref=target.at[pl.ds(part * pages, pages), head],
            send_sem=send_sem.at[step, k],
            recv_sem=recv_sem.at[index, k],
            device_id=(owner, dest_of(step)),
            device_id_type=MESH,
        )

    def local(step, k):
        source, target = trio[k]
        return pltpu.make_async_copy(source.at[step], target.at[pl.ds(part * pages, pages), head], own_sem.at[k])

    def work(step, carry):
        @pl.when(step + SLOTS - 1 < seqs)
        def _():
            fetch(step + SLOTS - 1)

        slot = lax.rem(step, SLOTS)
        dest = dest_of(step)
        for t in range(PAGE):
            pltpu.make_async_copy(keys.at[dest, :, t], buf.at[slot, t], key_sem.at[slot, t]).wait()
        block = buf.at[slot]
        flat = block.reshape(PAGE, rows, lanes)
        limit = lengths[dest] - seq * (pages * PAGE)
        row = lax.broadcasted_iota(jnp.int32, (chunk, lanes), 0)
        token = (row // width) * PAGE
        low_flat = low.at[step].reshape(rows, lanes)
        high_flat = high.at[step].reshape(rows, lanes)
        code_flat = code.at[step].reshape(rows, lanes)

        def piece(c, carry):
            at = pl.ds(pl.multiple_of(c * chunk, chunk), chunk)
            left = limit - c * (chunk // width * PAGE)
            small = jnp.full((chunk, lanes), jnp.inf, jnp.float32)
            large = jnp.full((chunk, lanes), -jnp.inf, jnp.float32)
            total = jnp.zeros((chunk, lanes), jnp.float32)
            for t in range(PAGE):
                x = flat[t, at, :].astype(jnp.float32)
                keep = token < left - t
                small = jnp.where(keep, jnp.minimum(small, x), small)
                large = jnp.where(keep, jnp.maximum(large, x), large)
                total = jnp.where(keep, total + x, total)
            live = token < left
            small = jnp.where(live, small, 0.0)
            large = jnp.where(live, large, 0.0)
            bound = jnp.maximum(jnp.abs(small), jnp.abs(large))
            share = jnp.abs(total) / (PAGE * jnp.where(bound > 0.0, bound, 1.0))
            level = jnp.log2(jnp.maximum(share, 1e-30)) * (TOP / SPAN) + TOP
            level = jnp.clip(level + 0.5, 0.0, TOP)
            level = jnp.where(total < 0.0, -level, level)
            low_flat[at, :] = small.astype(low.dtype)
            high_flat[at, :] = large.astype(high.dtype)
            code_flat[at, :] = level.astype(jnp.int32).astype(jnp.int16)
            return carry

        lax.fori_loop(0, rows // chunk, piece, 0)
        itself = jnp.logical_and(mine, dest == seq)

        @pl.when(itself)
        def _():
            for k in range(3):
                local(step, k).start()

        @pl.when(jnp.logical_not(itself))
        def _():
            for k in range(3):
                remote(step, k).start()

        return carry

    lax.fori_loop(0, seqs, work, 0)

    for i in range(heads - 1):
        query_copy(i, lax.rem(head + i + 1, heads)).wait()
    own_query.wait()

    def finish(step, carry):
        itself = jnp.logical_and(mine, dest_of(step) == seq)

        @pl.when(itself)
        def _():
            for k in range(3):
                local(step, k).wait()

        @pl.when(jnp.logical_not(itself))
        def _():
            for k in range(3):
                remote(step, k).wait_send()

        return carry

    lax.fori_loop(0, seqs, finish, 0)

    def arrive(i, carry):
        source_head = i // ratio
        source_part = lax.rem(i, ratio)
        itself = jnp.logical_and(source_head == head, head * ratio + source_part == seq)

        @pl.when(jnp.logical_not(itself))
        def _():
            for k in range(3):
                source, target = trio[k]
                pltpu.make_async_remote_copy(
                    src_ref=source.at[0],
                    dst_ref=target.at[pl.ds(source_part * pages, pages), source_head],
                    send_sem=send_sem.at[0, k],
                    recv_sem=recv_sem.at[i, k],
                    device_id=(source_head, head * ratio + source_part),
                    device_id_type=MESH,
                ).wait_recv()

        return carry

    lax.fori_loop(0, seqs, arrive, 0)


def score_kernel(lengths, low, high, code, query, low_out, high_out, mean_out, score_out):
    block, kv_heads, lanes = low.shape
    count_q = query.shape[0]
    total_pages = block * pl.num_programs(0)
    start = lax.axis_index("head") * total_pages + pl.program_id(0) * block
    limit = lengths[lax.axis_index("seq")]
    small = low[...]
    large = high[...]
    low_out[0] = small
    high_out[0] = large
    bound = jnp.maximum(jnp.abs(small.astype(jnp.float32)), jnp.abs(large.astype(jnp.float32)))
    level = code[...].astype(jnp.int32).astype(jnp.float32)
    share = jnp.exp2((jnp.abs(level) - TOP) * (SPAN / TOP))
    total = jnp.where(level == 0.0, 0.0, share * (PAGE * bound))
    total = jnp.where(level < 0.0, -total, total)
    page = start + lax.broadcasted_iota(jnp.int32, (block, kv_heads, lanes), 0)
    count = jnp.clip(limit - page * PAGE, 1, PAGE).astype(jnp.float32)
    mean_out[0] = total / count
    q = query[...].astype(jnp.float32)
    positive = jnp.maximum(q, 0.0).astype(jnp.bfloat16)
    negative = jnp.minimum(q, 0.0).astype(jnp.bfloat16)
    dims = (((1,), (1,)), ((), ()))
    both = lax.dot_general(
        large.reshape(block * kv_heads, lanes), positive, dims, preferred_element_type=jnp.float32
    ) + lax.dot_general(
        small.reshape(block * kv_heads, lanes), negative, dims, preferred_element_type=jnp.float32
    )
    both = both.reshape(block, kv_heads, count_q)
    kv = lax.broadcasted_iota(jnp.int32, both.shape, 1)
    of = lax.broadcasted_iota(jnp.int32, both.shape, 2) // (count_q // kv_heads)
    score = jnp.sum(jnp.where(kv == of, both, 0.0), axis=1) * lanes ** (-0.5)
    score_out[0] = score.T


def local_step(heads, seqs, cached_keys, queries, seq_lengths):
    seq_count, tokens, width, lanes = cached_keys.shape
    pages = tokens // PAGE
    owned = pages * seqs // heads
    local_q = queries.shape[1]
    keys = cached_keys.reshape(seq_count, pages, PAGE, width, lanes)
    any_space = pl.BlockSpec(memory_space=pl.ANY)
    shape = (owned, heads, width, lanes)
    low, high, code, query = pl.pallas_call(
        functools.partial(page_kernel, seqs, heads),
        out_shape=(
            jax.ShapeDtypeStruct(shape, jnp.bfloat16),
            jax.ShapeDtypeStruct(shape, jnp.bfloat16),
            jax.ShapeDtypeStruct(shape, jnp.int16),
            jax.ShapeDtypeStruct((heads, local_q, lanes), jnp.bfloat16),
        ),
        in_specs=[pl.BlockSpec(memory_space=pltpu.SMEM), any_space, any_space],
        out_specs=(any_space,) * 4,
        scratch_shapes=[
            pltpu.VMEM((SLOTS, PAGE, pages, width, lanes), jnp.bfloat16),
            pltpu.VMEM((seqs, pages, width, lanes), jnp.bfloat16),
            pltpu.VMEM((seqs, pages, width, lanes), jnp.bfloat16),
            pltpu.VMEM((seqs, pages, width, lanes), jnp.int16),
            pltpu.SemaphoreType.DMA((SLOTS, PAGE)),
            pltpu.SemaphoreType.DMA((seqs, 3)),
            pltpu.SemaphoreType.DMA((seqs, 3)),
            pltpu.SemaphoreType.DMA((3,)),
            pltpu.SemaphoreType.DMA((heads - 1,)),
            pltpu.SemaphoreType.DMA((heads - 1,)),
            pltpu.SemaphoreType.DMA,
        ],
        compiler_params=pltpu.CompilerParams(collective_id=0, has_side_effects=True),
        name="page_exchange",
    )(seq_lengths, keys, queries.reshape(local_q, lanes))
    kv_heads = heads * width
    count_q = heads * local_q
    block = min(128, owned)
    page_spec = pl.BlockSpec((block, kv_heads, lanes), lambda i: (i, 0, 0))
    out_spec = pl.BlockSpec((1, block, kv_heads, lanes), lambda i: (0, i, 0, 0))
    whole = (1, owned, kv_heads, lanes)
    return pl.pallas_call(
        score_kernel,
        grid=(owned // block,),
        out_shape=(
            jax.ShapeDtypeStruct(whole, jnp.bfloat16),
            jax.ShapeDtypeStruct(whole, jnp.bfloat16),
            jax.ShapeDtypeStruct(whole, jnp.float32),
            jax.ShapeDtypeStruct((1, count_q, owned), jnp.float32),
        ),
        in_specs=[
            pl.BlockSpec(memory_space=pltpu.SMEM),
            page_spec,
            page_spec,
            page_spec,
            pl.BlockSpec((count_q, lanes), lambda i: (0, 0)),
        ],
        out_specs=(out_spec, out_spec, out_spec, pl.BlockSpec((1, count_q, block), lambda i: (0, 0, i))),
        name="page_score",
    )(
        seq_lengths,
        low.reshape(owned, kv_heads, lanes),
        high.reshape(owned, kv_heads, lanes),
        code.reshape(owned, kv_heads, lanes),
        query.reshape(count_q, lanes),
    )


def solution(mesh):
    return jax.shard_map(
        functools.partial(local_step, mesh.shape["head"], mesh.shape["seq"]),
        mesh=mesh,
        in_specs=(P(None, "seq", "head", None), P("seq", "head", None), P()),
        out_specs=(
            P("seq", "head", None, None),
            P("seq", "head", None, None),
            P("seq", "head", None, None),
            P("seq", None, "head"),
        ),
        check_vma=False,
    )
```

```python
import functools

import jax
import jax.numpy as jnp
from jax import lax
from jax.experimental import pallas as pl
from jax.experimental.pallas import tpu as pltpu
from jax.sharding import PartitionSpec as P

PAGE = 16
SLOTS = 3
MESH = pl.DeviceIdType.MESH
SPAN = 28.0
TOP = 32767.0


def page_kernel(
    seqs, heads, lengths, keys, query, low_out, high_out, sum_out, query_out,
    buf, low, high, code, key_sem, send_sem, recv_sem, own_sem, query_send, query_recv, query_own,
):
    head = lax.axis_index("head")
    seq = lax.axis_index("seq")
    ratio = seqs // heads
    pages = keys.shape[1]
    width = keys.shape[3]
    lanes = keys.shape[4]
    rows = pages * width
    chunk = min(64, rows)
    owner = seq // ratio
    part = lax.rem(seq, ratio)
    mine = owner == head

    upper = owner >= (heads + 1) // 2
    from_end = jnp.where(upper, heads - 1 - owner, owner)

    def dest_of(step):
        turn = step // ratio
        ahead = heads - 1 - from_end
        plane = jnp.where(turn < ahead, from_end + 1 + turn, jnp.where(turn < heads - 1, heads - 2 - turn, from_end))
        plane = jnp.where(upper, heads - 1 - plane, plane)
        return plane * ratio + lax.rem(part + step, ratio)

    def fetch(step):
        slot = lax.rem(step, SLOTS)
        dest = dest_of(step)
        for t in range(PAGE):
            pltpu.make_async_copy(keys.at[dest, :, t], buf.at[slot, t], key_sem.at[slot, t]).start()

    for step in range(min(SLOTS - 1, seqs)):
        fetch(jnp.int32(step))

    barrier = pltpu.get_barrier_semaphore()

    def greet(i, carry):
        source_head = i // ratio
        source_seq = head * ratio + lax.rem(i, ratio)

        @pl.when(jnp.logical_or(source_head != head, source_seq != seq))
        def _():
            pl.semaphore_signal(barrier, inc=1, device_id=(source_head, source_seq), device_id_type=MESH)

        return carry

    lax.fori_loop(0, seqs, greet, 0)
    for i in range(1, heads):
        pl.semaphore_signal(barrier, inc=1, device_id=(lax.rem(head + i, heads), seq), device_id_type=MESH)
    expected = seqs - jnp.where(mine, 1, 0) + heads - 1
    pl.semaphore_wait(barrier, expected)

    def query_copy(i, target):
        return pltpu.make_async_remote_copy(
            src_ref=query, dst_ref=query_out.at[head], send_sem=query_send.at[i], recv_sem=query_recv.at[i],
            device_id=(target, seq), device_id_type=MESH,
        )

    for i in range(heads - 1):
        query_copy(i, lax.rem(head + i + 1, heads)).start()
    own_query = pltpu.make_async_copy(query, query_out.at[head], query_own)
    own_query.start()

    trio = ((low, low_out), (high, high_out), (code, sum_out))
    index = head * ratio + part

    def remote(step, k):
        source, target = trio[k]
        return pltpu.make_async_remote_copy(
            src_ref=source.at[step],
            dst_ref=target.at[pl.ds(part * pages, pages), head],
            send_sem=send_sem.at[step, k],
            recv_sem=recv_sem.at[index, k],
            device_id=(owner, dest_of(step)),
            device_id_type=MESH,
        )

    def local(step, k):
        source, target = trio[k]
        return pltpu.make_async_copy(source.at[step], target.at[pl.ds(part * pages, pages), head], own_sem.at[k])

    def work(step, carry):
        @pl.when(step + SLOTS - 1 < seqs)
        def _():
            fetch(step + SLOTS - 1)

        slot = lax.rem(step, SLOTS)
        dest = dest_of(step)
        for t in range(PAGE):
            pltpu.make_async_copy(keys.at[dest, :, t], buf.at[slot, t], key_sem.at[slot, t]).wait()
        block = buf.at[slot]
        flat = block.reshape(PAGE, rows, lanes)
        limit = lengths[dest] - seq * (pages * PAGE)
        row = lax.broadcasted_iota(jnp.int32, (chunk, lanes), 0)
        token = (row // width) * PAGE
        low_flat = low.at[step].reshape(rows, lanes)
        high_flat = high.at[step].reshape(rows, lanes)
        code_flat = code.at[step].reshape(rows, lanes)

        def piece(c, carry):
            at = pl.ds(pl.multiple_of(c * chunk, chunk), chunk)
            left = limit - c * (chunk // width * PAGE)
            small = jnp.full((chunk, lanes), jnp.inf, jnp.float32)
            large = jnp.full((chunk, lanes), -jnp.inf, jnp.float32)
            total = jnp.zeros((chunk, lanes), jnp.float32)
            for t in range(PAGE):
                x = flat[t, at, :].astype(jnp.float32)
                keep = token < left - t
                small = jnp.where(keep, jnp.minimum(small, x), small)
                large = jnp.where(keep, jnp.maximum(large, x), large)
                total = jnp.where(keep, total + x, total)
            live = token < left
            small = jnp.where(live, small, 0.0)
            large = jnp.where(live, large, 0.0)
            bound = jnp.maximum(jnp.abs(small), jnp.abs(large))
            share = jnp.abs(total) / (PAGE * jnp.where(bound > 0.0, bound, 1.0))
            level = jnp.log2(jnp.maximum(share, 1e-30)) * (TOP / SPAN) + TOP
            level = jnp.clip(level + 0.5, 0.0, TOP)
            level = jnp.where(total < 0.0, -level, level)
            low_flat[at, :] = small.astype(low.dtype)
            high_flat[at, :] = large.astype(high.dtype)
            code_flat[at, :] = level.astype(jnp.int32).astype(jnp.int16)
            return carry

        lax.fori_loop(0, rows // chunk, piece, 0)
        itself = jnp.logical_and(mine, dest == seq)

        @pl.when(itself)
        def _():
            for k in range(3):
                local(step, k).start()

        @pl.when(jnp.logical_not(itself))
        def _():
            for k in range(3):
                remote(step, k).start()

        return carry

    lax.fori_loop(0, seqs, work, 0)

    for i in range(heads - 1):
        query_copy(i, lax.rem(head + i + 1, heads)).wait()
    own_query.wait()

    def finish(step, carry):
        itself = jnp.logical_and(mine, dest_of(step) == seq)

        @pl.when(itself)
        def _():
            for k in range(3):
                local(step, k).wait()

        @pl.when(jnp.logical_not(itself))
        def _():
            for k in range(3):
                remote(step, k).wait_send()

        return carry

    lax.fori_loop(0, seqs, finish, 0)

    def arrive(i, carry):
        source_head = i // ratio
        source_part = lax.rem(i, ratio)
        itself = jnp.logical_and(source_head == head, head * ratio + source_part == seq)

        @pl.when(jnp.logical_not(itself))
        def _():
            for k in range(3):
                source, target = trio[k]
                pltpu.make_async_remote_copy(
                    src_ref=source.at[0],
                    dst_ref=target.at[pl.ds(source_part * pages, pages), source_head],
                    send_sem=send_sem.at[0, k],
                    recv_sem=recv_sem.at[i, k],
                    device_id=(source_head, head * ratio + source_part),
                    device_id_type=MESH,
                ).wait_recv()

        return carry

    lax.fori_loop(0, seqs, arrive, 0)


def score_kernel(lengths, low, high, code, query, low_out, high_out, mean_out, score_out):
    block, kv_heads, lanes = low.shape
    count_q = query.shape[0]
    total_pages = block * pl.num_programs(0)
    start = lax.axis_index("head") * total_pages + pl.program_id(0) * block
    limit = lengths[lax.axis_index("seq")]
    small = low[...]
    large = high[...]
    low_out[0] = small
    high_out[0] = large
    bound = jnp.maximum(jnp.abs(small.astype(jnp.float32)), jnp.abs(large.astype(jnp.float32)))
    level = code[...].astype(jnp.int32).astype(jnp.float32)
    share = jnp.exp2((jnp.abs(level) - TOP) * (SPAN / TOP))
    total = jnp.where(level == 0.0, 0.0, share * (PAGE * bound))
    total = jnp.where(level < 0.0, -total, total)
    page = start + lax.broadcasted_iota(jnp.int32, (block, kv_heads, lanes), 0)
    count = jnp.clip(limit - page * PAGE, 1, PAGE).astype(jnp.float32)
    mean_out[0] = total / count
    q = query[...].astype(jnp.float32)
    positive = jnp.maximum(q, 0.0).astype(jnp.bfloat16)
    negative = jnp.minimum(q, 0.0).astype(jnp.bfloat16)
    dims = (((1,), (1,)), ((), ()))
    both = lax.dot_general(
        large.reshape(block * kv_heads, lanes), positive, dims, preferred_element_type=jnp.float32
    ) + lax.dot_general(
        small.reshape(block * kv_heads, lanes), negative, dims, preferred_element_type=jnp.float32
    )
    both = both.reshape(block, kv_heads, count_q)
    kv = lax.broadcasted_iota(jnp.int32, both.shape, 1)
    of = lax.broadcasted_iota(jnp.int32, both.shape, 2) // (count_q // kv_heads)
    score = jnp.sum(jnp.where(kv == of, both, 0.0), axis=1) * lanes ** (-0.5)
    score_out[0] = score.T


def local_step(heads, seqs, cached_keys, queries, seq_lengths):
    seq_count, tokens, width, lanes = cached_keys.shape
    pages = tokens // PAGE
    owned = pages * seqs // heads
    local_q = queries.shape[1]
    keys = cached_keys.reshape(seq_count, pages, PAGE, width, lanes)
    any_space = pl.BlockSpec(memory_space=pl.ANY)
    shape = (owned, heads, width, lanes)
    low, high, code, query = pl.pallas_call(
        functools.partial(page_kernel, seqs, heads),
        out_shape=(
            jax.ShapeDtypeStruct(shape, jnp.bfloat16),
            jax.ShapeDtypeStruct(shape, jnp.bfloat16),
            jax.ShapeDtypeStruct(shape, jnp.int16),
            jax.ShapeDtypeStruct((heads, local_q, lanes), jnp.bfloat16),
        ),
        in_specs=[pl.BlockSpec(memory_space=pltpu.SMEM), any_space, any_space],
        out_specs=(any_space,) * 4,
        scratch_shapes=[
            pltpu.VMEM((SLOTS, PAGE, pages, width, lanes), jnp.bfloat16),
            pltpu.VMEM((seqs, pages, width, lanes), jnp.bfloat16),
            pltpu.VMEM((seqs, pages, width, lanes), jnp.bfloat16),
            pltpu.VMEM((seqs, pages, width, lanes), jnp.int16),
            pltpu.SemaphoreType.DMA((SLOTS, PAGE)),
            pltpu.SemaphoreType.DMA((seqs, 3)),
            pltpu.SemaphoreType.DMA((seqs, 3)),
            pltpu.SemaphoreType.DMA((3,)),
            pltpu.SemaphoreType.DMA((heads - 1,)),
            pltpu.SemaphoreType.DMA((heads - 1,)),
            pltpu.SemaphoreType.DMA,
        ],
        compiler_params=pltpu.CompilerParams(collective_id=0, has_side_effects=True),
        name="page_exchange",
    )(seq_lengths, keys, queries.reshape(local_q, lanes))
    kv_heads = heads * width
    count_q = heads * local_q
    block = min(128, owned)
    page_spec = pl.BlockSpec((block, kv_heads, lanes), lambda i: (i, 0, 0))
    out_spec = pl.BlockSpec((1, block, kv_heads, lanes), lambda i: (0, i, 0, 0))
    whole = (1, owned, kv_heads, lanes)
    return pl.pallas_call(
        score_kernel,
        grid=(owned // block,),
        out_shape=(
            jax.ShapeDtypeStruct(whole, jnp.bfloat16),
            jax.ShapeDtypeStruct(whole, jnp.bfloat16),
            jax.ShapeDtypeStruct(whole, jnp.float32),
            jax.ShapeDtypeStruct((1, count_q, owned), jnp.float32),
        ),
        in_specs=[
            pl.BlockSpec(memory_space=pltpu.SMEM),
            page_spec,
            page_spec,
            page_spec,
            pl.BlockSpec((count_q, lanes), lambda i: (0, 0)),
        ],
        out_specs=(out_spec, out_spec, out_spec, pl.BlockSpec((1, count_q, block), lambda i: (0, 0, i))),
        name="page_score",
    )(
        seq_lengths,
        low.reshape(owned, kv_heads, lanes),
        high.reshape(owned, kv_heads, lanes),
        code.reshape(owned, kv_heads, lanes),
        query.reshape(count_q, lanes),
    )


def solution(mesh):
    return jax.shard_map(
        functools.partial(local_step, mesh.shape["head"], mesh.shape["seq"]),
        mesh=mesh,
        in_specs=(P(None, "seq", "head", None), P("seq", "head", None), P()),
        out_specs=(
            P("seq", "head", None, None),
            P("seq", "head", None, None),
            P("seq", "head", None, None),
            P("seq", None, "head"),
        ),
        check_vma=False,
    )
```
